32 devices in a mesh: row: 4 (over x, core), col: 8 (over z, y).
Axes of the slice: x: 2, y: 2, z: 4, core: 2. Of those that a mesh axis runs over, the one named last changes fastest.
Arguments:
- fock_matrix: float32 [4096, 4096], P('row', 'col'), as said below
- density: float32 [4096, 4096], P('row', 'col'), as said below
- basis_gram: float32 [4096, 4096], P('row', 'col'), as said below
- error_history: float32 [6, 4096, 4096], P(None, 'row', 'col'), as said below
- fock_history: float32 [6, 4096, 4096], P(None, 'row', 'col'), may hold values from -6 to 6
Outputs:
- fock_next: float32 [4096, 4096], P('row', 'col')
- error_new: float32 [4096, 4096], P('row', 'col')
- weights: float32 [7], replicated
The draws below stay inside these ranges and needn't reach their ends.
Inputs may be any that keep to these rules, and one draw needn't show every extreme that they name: `fock_matrix`: symmetric. `density`: symmetric. `basis_gram`: symmetric. `error_history`: each of the 6 matrices is antisymmetric.
All inputs are finite; a program needn't handle non-finite values.
Results may differ from the reference program's by a relative error of at most 0.000098.
Values sent between devices are 32-bit elements; how exact they have to be, the bound alone decides.
A program may use at most 128 MiB of HBM per device.

```python
import jax
import jax.numpy as jnp
from jax import lax

N = 4096
HIST = 6


def draw_fock_matrix(key, part):
    base = jax.random.normal(jax.random.fold_in(key, 11), (N, N), jnp.float32)
    return (base + base.T) * 0.7071


def draw_density(key, part):
    base = jax.random.normal(jax.random.fold_in(key, 21), (N, N), jnp.float32)
    return (base + base.T) * (0.7071 / N ** 0.5)


def draw_basis_gram(key, part):
    base = jax.random.normal(jax.random.fold_in(key, 31), (N, N), jnp.float32)
    return jnp.eye(N, dtype=jnp.float32) + (base + base.T) * (0.35 / N ** 0.5)


def draw_error_history(key, part):
    common = jax.random.normal(jax.random.fold_in(key, 41), (N, N), jnp.float32)
    own = jax.random.normal(jax.random.fold_in(key, 42), (HIST, N, N), jnp.float32)
    spread = 0.7
    scales = jnp.exp(jax.random.uniform(jax.random.fold_in(key, 43), (HIST, 1, 1), jnp.float32, -spread, spread))
    mixed = (0.6 * common[None] + 0.8 * own) * scales
    return (mixed - jnp.swapaxes(mixed, 1, 2)) * 0.7071


def levels(rng, dims, shards, low, high):
    factor_of, own = 1.0, jax.random.fold_in(rng, 6)
    for position, parts in shards:
        steps = jnp.exp(jax.random.uniform(jax.random.fold_in(own, position), (parts,), jnp.float32, low / len(shards), high / len(shards)))
        factor_of = factor_of * jnp.repeat(steps, dims[position] // parts).reshape([-1 if axis == position else 1 for axis in range(len(dims))])
    return factor_of


def normal_values(stream_key, dims, width, most, pieces=(), kind=jnp.bfloat16):
    values = jax.random.normal(stream_key, dims, jnp.float32) * width
    if len(pieces) > 0:
        values = levels(stream_key, dims, pieces, -0.22, 0.18) * values
    return jnp.clip(values, min=-most, max=most).astype(kind)


def setup_inputs(seed: int = 0) -> dict:
    key_of = jax.random.split(jax.random.key(seed), 6)
    return {
        "fock_matrix": draw_fock_matrix(jax.random.fold_in(key_of[5], 71), 0),
        "density": draw_density(jax.random.fold_in(key_of[5], 71), 0),
        "basis_gram": draw_basis_gram(jax.random.fold_in(key_of[5], 71), 0),
        "error_history": draw_error_history(jax.random.fold_in(key_of[5], 71), 0),
        "fock_history": normal_values(key_of[4], (HIST, N, N), 1.0, 6.0, ((1, 4), (2, 8)), jnp.float32),
    }


def solve_weights(gram):
    size = gram.shape[0]
    factor = jnp.linalg.cholesky(gram)
    forward = []
    for index in range(size):
        total = jnp.float32(1.0)
        for inner in range(index):
            total = total - factor[index, inner] * forward[inner]
        forward.append(total / factor[index, index])
    backward = [None] * size
    for index in range(size - 1, -1, -1):
        total = forward[index]
        for inner in range(index + 1, size):
            total = total - factor[inner, index] * backward[inner]
        backward[index] = total / factor[index, index]
    solved = jnp.stack(backward)
    return solved / jnp.sum(solved)

def reference(fock_matrix, density, basis_gram, error_history, fock_history):
    highest = lax.Precision.HIGHEST
    middle = jnp.dot(density.astype(jnp.float32), basis_gram.astype(jnp.float32), precision=highest, preferred_element_type=jnp.float32)
    product = jnp.dot(fock_matrix.astype(jnp.float32), middle.astype(jnp.float32), precision=highest, preferred_element_type=jnp.float32)
    error_new = product - product.T
    stacked = jnp.concatenate([error_history, error_new[None]], axis=0)
    gram = jnp.einsum('kij,lij->kl', stacked, stacked, precision=highest)
    weights = solve_weights(gram)
    fock_next = jnp.einsum('k,kij->ij', weights[:HIST], fock_history, precision=highest) + weights[HIST] * fock_matrix
    return (fock_next, error_new, weights)
```

```python
import functools

import jax
import jax.numpy as jnp
from jax import lax
from jax.experimental import pallas as pl
from jax.experimental.pallas import tpu as pltpu
from jax.sharding import PartitionSpec as P


def gather_rows(block):
    size = lax.axis_size("row")
    depth = block.shape[0]
    mine = lax.axis_index("row")
    whole = jnp.zeros((size * depth, block.shape[1]), block.dtype)
    whole = lax.dynamic_update_slice_in_dim(whole, block, mine * depth, 0)
    for mask in range(1, size):
        pairs = [(source, source ^ mask) for source in range(size)]
        arrived = lax.ppermute(block, "row", pairs)
        whole = lax.dynamic_update_slice_in_dim(whole, arrived, (mine ^ mask) * depth, 0)
    return whole


def history_kernel(err_ref, out_ref):
    count = err_ref.shape[0]

    @pl.when(pl.program_id(0) == 0)
    def _():
        out_ref[...] = jnp.zeros_like(out_ref)

    tiles = err_ref.shape[1] // 8
    width = err_ref.shape[2]
    pairs = [(i, j) for i in range(count) for j in range(i, count)]

    def step(t, sums):
        rows = pl.ds(pl.multiple_of(t * 8, 8), 8)
        vals = [err_ref[k, rows, :] for k in range(count)]
        new = []
        for total, (i, j) in zip(sums, pairs):
            prod = vals[i] * vals[j]
            for c in range(0, width, 128):
                total = total + prod[:, c : c + 128]
            new.append(total)
        return tuple(new)

    zero = jnp.zeros((8, 128), jnp.float32)
    sums = lax.fori_loop(0, tiles, step, (zero,) * len(pairs))
    for total, (i, j) in zip(sums, pairs):
        out_ref[i * count + j] += total


def history_sums(errors):
    count, rows, width = errors.shape
    tile = min(rows, 128)
    out = pl.pallas_call(
        history_kernel,
        grid=(rows // tile,),
        in_specs=[pl.BlockSpec((count, tile, width), lambda i: (0, i, 0))],
        out_specs=pl.BlockSpec((count * count, 8, 128), lambda i: (0, 0, 0)),
        out_shape=jax.ShapeDtypeStruct((count * count, 8, 128), jnp.float32),
        cost_estimate=pl.CostEstimate(flops=42 * rows * width, bytes_accessed=errors.size * 4, transcendentals=0),
        name="history_sums",
    )(errors)
    upper = jnp.sum(out, axis=(1, 2)).reshape(count, count)
    return jnp.triu(upper) + jnp.triu(upper, 1).T


def cross_kernel(err_ref, prod_ref, out_ref):
    count = err_ref.shape[0]

    @pl.when(pl.program_id(0) == 0)
    def _():
        out_ref[...] = jnp.zeros_like(out_ref)

    tiles = err_ref.shape[1] // 8
    width = err_ref.shape[2]

    def step(t, sums):
        rows = pl.ds(pl.multiple_of(t * 8, 8), 8)
        prod = prod_ref[rows, :]
        new = []
        for k in range(count):
            term = err_ref[k, rows, :] * prod
            total = sums[k]
            for c in range(0, width, 128):
                total = total + term[:, c : c + 128]
            new.append(total)
        return tuple(new)

    zero = jnp.zeros((8, 128), jnp.float32)
    sums = lax.fori_loop(0, tiles, step, (zero,) * count)
    for k in range(count):
        out_ref[k] += sums[k]


def cross_sums(errors, product):
    count, rows, width = errors.shape
    tile = min(rows, 128)
    out = pl.pallas_call(
        cross_kernel,
        grid=(rows // tile,),
        in_specs=[
            pl.BlockSpec((count, tile, width), lambda i: (0, i, 0)),
            pl.BlockSpec((tile, width), lambda i: (i, 0)),
        ],
        out_specs=pl.BlockSpec((count, 8, 128), lambda i: (0, 0, 0)),
        out_shape=jax.ShapeDtypeStruct((count, 8, 128), jnp.float32),
        cost_estimate=pl.CostEstimate(flops=12 * rows * width, bytes_accessed=errors.size * 4, transcendentals=0),
        name="cross_sums",
    )(errors, product)
    return 2.0 * jnp.sum(out, axis=(1, 2))


def error_kernel(odd_ref, prod_ref, first_ref, second_ref, out_ref, sum_ref):
    step = pl.program_id(0)

    @pl.when(step == 0)
    def _():
        sum_ref[...] = jnp.zeros_like(sum_ref)

    odd = odd_ref[0]

    def finish(piece_ref):
        error = prod_ref[...] - piece_ref[...].T
        out_ref[...] = error
        squares = error * error
        rows, width = squares.shape
        total = jnp.sum(squares.reshape(rows // 8, 8, width), axis=0)
        acc = total[:, :128]
        for c in range(128, width, 128):
            acc = acc + total[:, c : c + 128]
        sum_ref[...] += acc

    @pl.when(step == odd)
    def _():
        finish(first_ref)

    @pl.when(step != odd)
    def _():
        finish(second_ref)


def subtract_mirror(odd, product, first, second):
    rows, width = product.shape
    error, sums = pl.pallas_call(
        error_kernel,
        grid=(2,),
        in_specs=[
            pl.BlockSpec(memory_space=pltpu.SMEM),
            pl.BlockSpec((width, width), lambda i: (i, 0)),
            pl.BlockSpec((width, width), lambda i: (0, 0)),
            pl.BlockSpec((width, width), lambda i: (0, 0)),
        ],
        out_specs=[
            pl.BlockSpec((width, width), lambda i: (i, 0)),
            pl.BlockSpec((8, 128), lambda i: (0, 0)),
        ],
        out_shape=[
            jax.ShapeDtypeStruct((rows, width), jnp.float32),
            jax.ShapeDtypeStruct((8, 128), jnp.float32),
        ],
        name="subtract_mirror",
    )(odd[None], product, first, second)
    return error, jnp.sum(sums)


def finish_kernel(gram_ref, hist_ref, fock_ref, out_ref, weights_ref, scaled):
    count = hist_ref.shape[0]
    size = count + 1

    @pl.when(pl.program_id(0) == 0)
    def _():
        full = lambda value: jnp.full((8, 128), value, jnp.float32)
        factor = [[None] * size for _ in range(size)]
        for j in range(size):
            diag = full(gram_ref[j, j])
            for k in range(j):
                diag = diag - factor[j][k] * factor[j][k]
            factor[j][j] = jnp.sqrt(diag)
            for i in range(j + 1, size):
                total = full(gram_ref[i, j])
                for k in range(j):
                    total = total - factor[i][k] * factor[j][k]
                factor[i][j] = total / factor[j][j]
        forward = []
        for i in range(size):
            total = full(1.0)
            for k in range(i):
                total = total - factor[i][k] * forward[k]
            forward.append(total / factor[i][i])
        solved = [None] * size
        for i in range(size - 1, -1, -1):
            total = forward[i]
            for k in range(i + 1, size):
                total = total - factor[k][i] * solved[k]
            solved[i] = total / factor[i][i]
        norm = solved[0]
        for i in range(1, size):
            norm = norm + solved[i]
        for i in range(size):
            scaled[i] = solved[i] / norm
            weights_ref[i] = scaled[i]

    rows, width = fock_ref.shape
    weights = [scaled[i] for i in range(size)]

    def step(t, carry):
        at = pl.ds(pl.multiple_of(t * 8, 8), 8)
        for c in range(0, width, 128):
            lanes = slice(c, c + 128)
            total = weights[count] * fock_ref[at, lanes]
            for k in range(count):
                total = total + weights[k] * hist_ref[k, at, lanes]
            out_ref[at, lanes] = total
        return carry

    lax.fori_loop(0, rows // 8, step, 0)


def combine(gram, history, fock):
    count, rows, width = history.shape
    tile = min(rows, 128)
    mixed, weights = pl.pallas_call(
        finish_kernel,
        grid=(rows // tile,),
        in_specs=[
            pl.BlockSpec(memory_space=pltpu.SMEM),
            pl.BlockSpec((count, tile, width), lambda i: (0, i, 0)),
            pl.BlockSpec((tile, width), lambda i: (i, 0)),
        ],
        out_specs=[
            pl.BlockSpec((tile, width), lambda i: (i, 0)),
            pl.BlockSpec((count + 1, 8, 128), lambda i: (0, 0, 0)),
        ],
        out_shape=[
            jax.ShapeDtypeStruct((rows, width), jnp.float32),
            jax.ShapeDtypeStruct((count + 1, 8, 128), jnp.float32),
        ],
        scratch_shapes=[pltpu.VMEM((count + 1, 8, 128), jnp.float32)],
        name="combine",
    )(gram, history, fock)
    return mixed, weights[:, 0, 0]


def body(fock_matrix, density, basis_gram, error_history, fock_history):
    high = lax.Precision.HIGH
    rows, width = fock_matrix.shape
    row_count, col_count = lax.axis_size("row"), lax.axis_size("col")
    col_index = lax.axis_index("col")
    odd = col_index % 2
    dens_rows = lax.all_gather(density, "col", axis=1, tiled=True)
    fock_rows = lax.all_gather(fock_matrix, "col", axis=1, tiled=True)
    gram_cols = gather_rows(basis_gram)
    history_local = history_sums(error_history)
    middle = jnp.dot(dens_rows, gram_cols, precision=high, preferred_element_type=jnp.float32)
    middle_cols = gather_rows(middle)
    product = jnp.dot(fock_rows, middle_cols, precision=high, preferred_element_type=jnp.float32)

    pieces = []
    for turn in range(2):
        start = (odd ^ turn) * width
        half = lax.dynamic_slice_in_dim(product, start, width, 0)
        pairs = []
        for r in range(row_count):
            for c in range(col_count):
                target = (c // 2, 2 * r + ((c % 2) ^ turn))
                pairs.append((r * col_count + c, target[0] * col_count + target[1]))
        pieces.append(lax.ppermute(half, ("row", "col"), pairs))
    cross_local = cross_sums(error_history, product)
    error_new, self_local = subtract_mirror(odd.astype(jnp.int32), product, pieces[0], pieces[1])
    history_gram, cross_terms, self_term = lax.psum((history_local, cross_local, self_local), ("row", "col"))
    upper = jnp.concatenate([history_gram, cross_terms[:, None]], axis=1)
    lower = jnp.concatenate([cross_terms, self_term[None]])[None, :]
    gram = jnp.concatenate([upper, lower], axis=0)
    fock_next, weights = combine(gram, fock_history, fock_matrix)
    return (fock_next, error_new, weights)


def solution(mesh):
    in_specs = (
        P("row", "col"),
        P("row", "col"),
        P("row", "col"),
        P(None, "row", "col"),
        P(None, "row", "col"),
    )
    out_specs = (P("row", "col"), P("row", "col"), P())
    return jax.shard_map(body, mesh=mesh, in_specs=in_specs, out_specs=out_specs, check_vma=False)
```

```python
import functools

import jax
import jax.numpy as jnp
from jax import lax
from jax.experimental import pallas as pl
from jax.experimental.pallas import tpu as pltpu
from jax.sharding import PartitionSpec as P


def gather_rows(block):
    size = lax.axis_size("row")
    depth = block.shape[0]
    mine = lax.axis_index("row")
    whole = jnp.zeros((size * depth, block.shape[1]), block.dtype)
    whole = lax.dynamic_update_slice_in_dim(whole, block, mine * depth, 0)
    for mask in range(1, size):
        pairs = [(source, source ^ mask) for source in range(size)]
        arrived = lax.ppermute(block, "row", pairs)
        whole = lax.dynamic_update_slice_in_dim(whole, arrived, (mine ^ mask) * depth, 0)
    return whole


def gather_columns(block):
    size = lax.axis_size("col")
    width = block.shape[1]
    mine = lax.axis_index("col")
    flip = [(source, source ^ 1) for source in range(size)]
    whole = jnp.zeros((block.shape[0], size * width), block.dtype)
    held = [(block, mine)]
    for shift in range(1, size // 2):
        pairs = [(source, (source + 2 * shift) % size) for source in range(size)]
        held.append((lax.ppermute(block, "col", pairs), (mine + size - 2 * shift) % size))
    for value, owner in held:
        other = lax.ppermute(value, "col", flip)
        whole = lax.dynamic_update_slice_in_dim(whole, value, owner * width, 1)
        whole = lax.dynamic_update_slice_in_dim(whole, other, (owner ^ 1) * width, 1)
    return whole


def history_kernel(err_ref, out_ref):
    count = err_ref.shape[0]

    @pl.when(pl.program_id(0) == 0)
    def _():
        out_ref[...] = jnp.zeros_like(out_ref)

    tiles = err_ref.shape[1] // 8
    width = err_ref.shape[2]
    pairs = [(i, j) for i in range(count) for j in range(i, count)]

    def step(t, sums):
        rows = pl.ds(pl.multiple_of(t * 8, 8), 8)
        vals = [err_ref[k, rows, :] for k in range(count)]
        new = []
        for total, (i, j) in zip(sums, pairs):
            prod = vals[i] * vals[j]
            for c in range(0, width, 128):
                total = total + prod[:, c : c + 128]
            new.append(total)
        return tuple(new)

    zero = jnp.zeros((8, 128), jnp.float32)
    sums = lax.fori_loop(0, tiles, step, (zero,) * len(pairs))
    for total, (i, j) in zip(sums, pairs):
        out_ref[i * count + j] += total


def history_sums(errors):
    count, rows, width = errors.shape
    tile = min(rows, 128)
    out = pl.pallas_call(
        history_kernel,
        grid=(rows // tile,),
        in_specs=[pl.BlockSpec((count, tile, width), lambda i: (0, i, 0))],
        out_specs=pl.BlockSpec((count * count, 8, 128), lambda i: (0, 0, 0)),
        out_shape=jax.ShapeDtypeStruct((count * count, 8, 128), jnp.float32),
        cost_estimate=pl.CostEstimate(flops=42 * rows * width, bytes_accessed=errors.size * 4, transcendentals=0),
        name="history_sums",
    )(errors)
    upper = jnp.sum(out, axis=(1, 2)).reshape(count, count)
    return jnp.triu(upper) + jnp.triu(upper, 1).T


def cross_kernel(err_ref, prod_ref, out_ref):
    count = err_ref.shape[0]

    @pl.when(pl.program_id(0) == 0)
    def _():
        out_ref[...] = jnp.zeros_like(out_ref)

    tiles = err_ref.shape[1] // 8
    width = err_ref.shape[2]

    def step(t, sums):
        rows = pl.ds(pl.multiple_of(t * 8, 8), 8)
        prod = prod_ref[rows, :]
        new = []
        for k in range(count):
            term = err_ref[k, rows, :] * prod
            total = sums[k]
            for c in range(0, width, 128):
                total = total + term[:, c : c + 128]
            new.append(total)
        return tuple(new)

    zero = jnp.zeros((8, 128), jnp.float32)
    sums = lax.fori_loop(0, tiles, step, (zero,) * count)
    for k in range(count):
        out_ref[k] += sums[k]


def cross_sums(errors, product):
    count, rows, width = errors.shape
    tile = min(rows, 128)
    out = pl.pallas_call(
        cross_kernel,
        grid=(rows // tile,),
        in_specs=[
            pl.BlockSpec((count, tile, width), lambda i: (0, i, 0)),
            pl.BlockSpec((tile, width), lambda i: (i, 0)),
        ],
        out_specs=pl.BlockSpec((count, 8, 128), lambda i: (0, 0, 0)),
        out_shape=jax.ShapeDtypeStruct((count, 8, 128), jnp.float32),
        cost_estimate=pl.CostEstimate(flops=12 * rows * width, bytes_accessed=errors.size * 4, transcendentals=0),
        name="cross_sums",
    )(errors, product)
    return 2.0 * jnp.sum(out, axis=(1, 2))


def error_kernel(odd_ref, prod_ref, first_ref, second_ref, out_ref, sum_ref):
    step = pl.program_id(0)

    @pl.when(step == 0)
    def _():
        sum_ref[...] = jnp.zeros_like(sum_ref)

    odd = odd_ref[0]

    def finish(piece_ref):
        error = prod_ref[...] - piece_ref[...].T
        out_ref[...] = error
        squares = error * error
        rows, width = squares.shape
        total = jnp.sum(squares.reshape(rows // 8, 8, width), axis=0)
        acc = total[:, :128]
        for c in range(128, width, 128):
            acc = acc + total[:, c : c + 128]
        sum_ref[...] += acc

    @pl.when(step == odd)
    def _():
        finish(first_ref)

    @pl.when(step != odd)
    def _():
        finish(second_ref)


def subtract_mirror(odd, product, first, second):
    rows, width = product.shape
    error, sums = pl.pallas_call(
        error_kernel,
        grid=(2,),
        in_specs=[
            pl.BlockSpec(memory_space=pltpu.SMEM),
            pl.BlockSpec((width, width), lambda i: (i, 0)),
            pl.BlockSpec((width, width), lambda i: (0, 0)),
            pl.BlockSpec((width, width), lambda i: (0, 0)),
        ],
        out_specs=[
            pl.BlockSpec((width, width), lambda i: (i, 0)),
            pl.BlockSpec((8, 128), lambda i: (0, 0)),
        ],
        out_shape=[
            jax.ShapeDtypeStruct((rows, width), jnp.float32),
            jax.ShapeDtypeStruct((8, 128), jnp.float32),
        ],
        name="subtract_mirror",
    )(odd[None], product, first, second)
    return error, jnp.sum(sums)


def finish_kernel(gram_ref, hist_ref, fock_ref, out_ref, weights_ref, scaled):
    count = hist_ref.shape[0]
    size = count + 1

    @pl.when(pl.program_id(0) == 0)
    def _():
        full = lambda value: jnp.full((8, 128), value, jnp.float32)
        factor = [[None] * size for _ in range(size)]
        for j in range(size):
            diag = full(gram_ref[j, j])
            for k in range(j):
                diag = diag - factor[j][k] * factor[j][k]
            factor[j][j] = jnp.sqrt(diag)
            for i in range(j + 1, size):
                total = full(gram_ref[i, j])
                for k in range(j):
                    total = total - factor[i][k] * factor[j][k]
                factor[i][j] = total / factor[j][j]
        forward = []
        for i in range(size):
            total = full(1.0)
            for k in range(i):
                total = total - factor[i][k] * forward[k]
            forward.append(total / factor[i][i])
        solved = [None] * size
        for i in range(size - 1, -1, -1):
            total = forward[i]
            for k in range(i + 1, size):
                total = total - factor[k][i] * solved[k]
            solved[i] = total / factor[i][i]
        norm = solved[0]
        for i in range(1, size):
            norm = norm + solved[i]
        for i in range(size):
            scaled[i] = solved[i] / norm
            weights_ref[i] = scaled[i]

    rows, width = fock_ref.shape
    weights = [scaled[i] for i in range(size)]

    def step(t, carry):
        at = pl.ds(pl.multiple_of(t * 8, 8), 8)
        for c in range(0, width, 128):
            lanes = slice(c, c + 128)
            total = weights[count] * fock_ref[at, lanes]
            for k in range(count):
                total = total + weights[k] * hist_ref[k, at, lanes]
            out_ref[at, lanes] = total
        return carry

    lax.fori_loop(0, rows // 8, step, 0)


def combine(gram, history, fock):
    count, rows, width = history.shape
    tile = min(rows, 128)
    mixed, weights = pl.pallas_call(
        finish_kernel,
        grid=(rows // tile,),
        in_specs=[
            pl.BlockSpec(memory_space=pltpu.SMEM),
            pl.BlockSpec((count, tile, width), lambda i: (0, i, 0)),
            pl.BlockSpec((tile, width), lambda i: (i, 0)),
        ],
        out_specs=[
            pl.BlockSpec((tile, width), lambda i: (i, 0)),
            pl.BlockSpec((count + 1, 8, 128), lambda i: (0, 0, 0)),
        ],
        out_shape=[
            jax.ShapeDtypeStruct((rows, width), jnp.float32),
            jax.ShapeDtypeStruct((count + 1, 8, 128), jnp.float32),
        ],
        scratch_shapes=[pltpu.VMEM((count + 1, 8, 128), jnp.float32)],
        name="combine",
    )(gram, history, fock)
    return mixed, weights[:, 0, 0]


def body(fock_matrix, density, basis_gram, error_history, fock_history):
    high = lax.Precision.HIGH
    rows, width = fock_matrix.shape
    row_count, col_count = lax.axis_size("row"), lax.axis_size("col")
    col_index = lax.axis_index("col")
    odd = col_index % 2
    dens_rows = lax.all_gather(density, "col", axis=1, tiled=True)
    fock_rows = gather_columns(fock_matrix)
    gram_cols = gather_rows(basis_gram)
    history_local = history_sums(error_history)
    middle = jnp.dot(dens_rows, gram_cols, precision=high, preferred_element_type=jnp.float32)
    middle_cols = gather_rows(middle)
    product = jnp.dot(fock_rows, middle_cols, precision=high, preferred_element_type=jnp.float32)

    pieces = []
    for turn in range(2):
        start = (odd ^ turn) * width
        half = lax.dynamic_slice_in_dim(product, start, width, 0)
        pairs = []
        for r in range(row_count):
            for c in range(col_count):
                target = (c // 2, 2 * r + ((c % 2) ^ turn))
                pairs.append((r * col_count + c, target[0] * col_count + target[1]))
        pieces.append(lax.ppermute(half, ("row", "col"), pairs))
    cross_local = cross_sums(error_history, product)
    error_new, self_local = subtract_mirror(odd.astype(jnp.int32), product, pieces[0], pieces[1])
    history_gram, cross_terms, self_term = lax.psum((history_local, cross_local, self_local), ("row", "col"))
    upper = jnp.concatenate([history_gram, cross_terms[:, None]], axis=1)
    lower = jnp.concatenate([cross_terms, self_term[None]])[None, :]
    gram = jnp.concatenate([upper, lower], axis=0)
    fock_next, weights = combine(gram, fock_history, fock_matrix)
    return (fock_next, error_new, weights)


def solution(mesh):
    in_specs = (
        P("row", "col"),
        P("row", "col"),
        P("row", "col"),
        P(None, "row", "col"),
        P(None, "row", "col"),
    )
    out_specs = (P("row", "col"), P("row", "col"), P())
    return jax.shard_map(body, mesh=mesh, in_specs=in_specs, out_specs=out_specs, check_vma=False)
```
